32 devices in a mesh: tm: 4 (over y, x), space: 8 (over z, core).
Axes of the slice: x: 2, y: 2, z: 4, core: 2. Of those that a mesh axis runs over, the one named last changes fastest.
Arguments:
- source: float32 [8, 1024, 5, 128], P('tm', 'space'), may hold values from -6 to 6
- terminal: float32 [1024, 5, 128], P('space'), may hold values from -6 to 6
- jacobian: float32 [4, 1024, 5, 5, 128], P('tm', 'space')
- face_coef: float32 [1024, 6, 128], P('space'), may hold values from 0.1 to 0.5
- cell_coef: float32 [1024, 128], P('space'), may hold values from 0.1 to 0.5
- neighbours: int32 [1024, 6], P('space'), may hold values from 0 to 160, as said below
- send_blocks: int32 [8, 2, 16], P('space'), may hold values from 0 to 127, as said below
- live_count: int32 [8], P('space'), may hold values from 64 to 128, as said below
- volume: float32 [1024, 128], P('space'), may hold values from 0.5 to 2
- shape_field: float32 [1024, 5, 128], P('space'), may hold values from -6 to 6
- weights: float32 [8], P('tm'), may hold values from 0.25 to 4
Outputs:
- adjoint: float32 [8, 1024, 5, 128], P('tm', 'space')
- sensitivity: float32 [1024], P('space')
The draws below stay inside these ranges and needn't reach their ends.
Inputs may be any that keep to these rules, and one draw needn't show every extreme that they name: `live_count`: some device has 128 live blocks in every draw. `send_blocks`: each index names a live block of its own device. `neighbours`: a slot below 128 names a live block of the same device; 128 to 159 name received blocks, those of the lower device first; 160 is an empty slot.
All inputs are finite; a program needn't handle non-finite values.
Results may differ from the reference program's by a relative error of at most 0.00016.
Values sent between devices are 32-bit elements; how exact they have to be, the bound alone decides.
A program may use at most 64 MiB of HBM per device.

```python
import math
import jax
import jax.numpy as jnp
from jax import lax

NB = 128
CELLS = 128
COMP = 5
NEI = 6
HALO = 16
STEPS = 2
ITERS = 3
BLOCKS = 1024
GROUPS = 4
TSTEPS = 8
N_SPACE = 8


def geometry(key):
    devices = BLOCKS // NB
    keys = jax.random.split(jax.random.fold_in(key, 17), 6)
    counts = jax.random.randint(keys[0], (devices,), NB // 2, NB + 1)
    fullest = jax.random.randint(keys[1], (), 0, devices)
    counts = counts.at[fullest].set(NB)
    sends = jax.random.randint(keys[2], (devices, 2, HALO), 0, 1 << 20) % counts[:, None, None]
    kinds = jax.random.randint(keys[3], (BLOCKS, NEI), 0, 6)
    block_counts = jnp.repeat(counts, NB)
    local = jax.random.randint(keys[4], (BLOCKS, NEI), 0, 1 << 20) % block_counts[:, None]
    remote = NB + jax.random.randint(keys[5], (BLOCKS, NEI), 0, 2 * HALO)
    table = jnp.where(kinds < 2, remote, jnp.where(kinds == 2, NB + 2 * HALO, local))
    return (counts.astype(jnp.int32), sends.astype(jnp.int32), table.astype(jnp.int32))


def draw_live_count(key, part):
    return geometry(key)[0]


def draw_send_blocks(key, part):
    return geometry(key)[1]


def draw_neighbours(key, part):
    return geometry(key)[2]


def draw_jacobian(key, part):
    first, second = jax.random.split(jax.random.fold_in(key, 29))
    shape = (GROUPS, BLOCKS, COMP, COMP, CELLS)
    identity = jnp.eye(COMP, dtype=jnp.float32)[None, None, :, :, None]
    off_part = 0.15 * jax.random.normal(first, shape, jnp.float32)
    diag_part = jax.random.uniform(second, shape, jnp.float32, 0.3, 1.0)
    return identity * diag_part + (1.0 - identity) * off_part


def block_scale(stream_key, shape, shards, smallest, top_value):
    gain, own = 1.0, jax.random.fold_in(stream_key, 6)
    for dim, shards_of in shards:
        draws = jnp.exp(jax.random.uniform(jax.random.fold_in(own, dim), (shards_of,), jnp.float32, smallest / len(shards), top_value / len(shards)))
        gain = gain * jnp.repeat(draws, shape[dim] // shards_of).reshape([-1 if axis == dim else 1 for axis in range(len(shape))])
    return gain


def scatter_about(stream_key, dims, spread, limit, cuts=(), kind=jnp.bfloat16):
    entries = spread * jax.random.normal(stream_key, dims, jnp.float32)
    if cuts:
        entries = entries * block_scale(stream_key, dims, cuts, -0.22, 0.18)
    return jnp.clip(entries, -limit, limit).astype(kind)


def setup_inputs(seed: int = 0) -> dict:
    arg_keys = jax.random.split(jax.random.key(seed), 12)
    source = scatter_about(arg_keys[0], (TSTEPS, BLOCKS, COMP, CELLS), 1.0, 6.0, ((0, 4), (1, 8)), jnp.float32)
    terminal = scatter_about(arg_keys[1], (BLOCKS, COMP, CELLS), 1.0, 6.0, ((0, 8),), jnp.float32)
    jacobian = draw_jacobian(jax.random.fold_in(arg_keys[11], 71), 0)
    face_coef = jnp.clip(0.1 + 0.4 * jax.random.uniform(arg_keys[3], (BLOCKS, NEI, CELLS), jnp.float32) ** block_scale(arg_keys[3], (BLOCKS, NEI, CELLS), ((0, 8),), -0.2, 0.2), 0.1, 0.5)
    cell_coef = jnp.clip(0.1 + 0.4 * jax.random.uniform(arg_keys[4], (BLOCKS, CELLS), jnp.float32) ** block_scale(arg_keys[4], (BLOCKS, CELLS), ((0, 8),), -0.2, 0.2), 0.1, 0.5)
    neighbours = draw_neighbours(jax.random.fold_in(arg_keys[11], 71), 0)
    send_blocks = draw_send_blocks(jax.random.fold_in(arg_keys[11], 71), 0)
    live_count = draw_live_count(jax.random.fold_in(arg_keys[11], 71), 0)
    volume = jnp.clip(jnp.exp(math.log(2.0) - 1.3862944 * jax.random.uniform(arg_keys[8], (BLOCKS, CELLS), jnp.float32) ** block_scale(arg_keys[8], (BLOCKS, CELLS), ((0, 8),), -0.2, 0.2)), 0.5, 2.0)
    shape_field = scatter_about(arg_keys[9], (BLOCKS, COMP, CELLS), 1.0, 6.0, ((0, 8),), jnp.float32)
    weights = jnp.clip(jnp.exp(math.log(4.0) - 2.7725887 * jax.random.uniform(arg_keys[10], (TSTEPS,), jnp.float32) ** block_scale(arg_keys[10], (TSTEPS,), ((0, 4),), -0.2, 0.2)), 0.25, 4.0)
    return {"source": source, "terminal": terminal, "jacobian": jacobian, "face_coef": face_coef, "cell_coef": cell_coef, "neighbours": neighbours, "send_blocks": send_blocks, "live_count": live_count, "volume": volume, "shape_field": shape_field, "weights": weights}


inverse_step = 6.0


def pick_rows(table, index):
    return table[index]


def reference(source, terminal, jacobian, face_coef, cell_coef, neighbours, send_blocks, live_count, volume, shape_field, weights):
    highest = lax.Precision.HIGHEST
    live = (jnp.arange(NB, dtype=jnp.int32)[None, :] < live_count[:, None]).astype(jnp.float32).reshape(BLOCKS, 1, 1)
    mass = (inverse_step * volume)[:, None, :]
    face_total = jnp.sum(face_coef, axis=1)[:, None, :]
    along_coef = cell_coef[:, None, :]
    neighbour_table = neighbours.reshape(N_SPACE, NB, NEI)

    def operate(field, jac):
        by_device = field.reshape(N_SPACE, NB, COMP, CELLS)
        to_lower = jax.vmap(pick_rows)(by_device, send_blocks[:, 0])
        to_higher = jax.vmap(pick_rows)(by_device, send_blocks[:, 1])
        zero_rim = jnp.zeros((1, HALO, COMP, CELLS), jnp.float32)
        from_lower = jnp.concatenate([zero_rim, to_higher[:-1]], axis=0)
        from_higher = jnp.concatenate([to_lower[1:], zero_rim], axis=0)
        blank = jnp.zeros((N_SPACE, 1, COMP, CELLS), jnp.float32)
        extended = jnp.concatenate([by_device, from_lower, from_higher, blank], axis=1)
        gathered = jax.vmap(pick_rows)(extended, neighbour_table).reshape(BLOCKS, NEI, COMP, CELLS)
        coupled = jnp.einsum("bnc,bnkc->bkc", face_coef, gathered, precision=highest)
        own = jnp.einsum("bijc,bic->bjc", jac, field, precision=highest)
        padded = jnp.pad(field, ((0, 0), (0, 0), (1, 1)))
        beside = padded[:, :, :-2] + padded[:, :, 2:]
        return mass * field + own - coupled - along_coef * beside

    later = live * terminal
    levels = []
    sensitivity = jnp.zeros((BLOCKS,), jnp.float32)
    for group in reversed(range(GROUPS)):
        jac = jacobian[group]
        diagonal = jnp.stack([jac[:, k, k, :] for k in range(COMP)], axis=1)
        precond = 1.0 / (mass + diagonal + face_total + 2.0 * along_coef)
        for level in reversed(range(STEPS)):
            index = group * STEPS + level
            rhs = source[index] + mass * later
            field = later
            for sweep in range(ITERS):
                field = live * (field + precond * (rhs - operate(field, jac)))
            levels.append(field)
            sensitivity = sensitivity + weights[index] * jnp.sum(field * shape_field, axis=(1, 2))
            later = field
    adjoint = jnp.stack(levels[::-1], axis=0)
    return adjoint, sensitivity
```

```python
import functools

import jax
import jax.numpy as jnp
from jax import lax
from jax.experimental import pallas as pl
from jax.experimental.pallas import tpu as pltpu
from jax.sharding import PartitionSpec as P

ITERS = 3
INVERSE_STEP = 6.0
UNROLL = 8


def kernel(
    groups,
    width,
    source_hbm,
    terminal_hbm,
    jac_hbm,
    face_hbm,
    cell_hbm,
    nbr,
    send_blocks,
    live_count,
    volume_hbm,
    shape_hbm,
    weights,
    adjoint_hbm,
    sens_ref,
    source,
    terminal,
    jac,
    face,
    cell,
    volume,
    shape,
    field,
    part,
    rate,
    rate_cell,
    rate_mass,
    rhs,
    levels,
    weighted,
    halo,
    edge,
    outbox,
    acc_in,
    acc_out,
    total,
    load_sem,
    store_sem,
    halo_send,
    halo_recv,
    state_send,
    state_recv,
    acc_send,
    acc_recv,
    total_send,
    total_recv,
):
    g = lax.axis_index("tm")
    d = lax.axis_index("space")
    steps, nb, comp, cells = source.shape
    nei = face.shape[1]
    count = outbox.shape[2]
    sweeps = steps * ITERS

    loads = [
        pltpu.make_async_copy(jac_hbm.at[0], jac, load_sem.at[0]),
        pltpu.make_async_copy(face_hbm, face, load_sem.at[1]),
        pltpu.make_async_copy(cell_hbm, cell, load_sem.at[2]),
        pltpu.make_async_copy(volume_hbm, volume, load_sem.at[3]),
        pltpu.make_async_copy(terminal_hbm, terminal, load_sem.at[4]),
        pltpu.make_async_copy(source_hbm, source, load_sem.at[5]),
        pltpu.make_async_copy(shape_hbm, shape, load_sem.at[6]),
    ]
    for load in loads:
        load.start()

    zero = jnp.zeros((comp, cells), jnp.float32)
    field[nb] = zero

    def clear(m, _):
        for row in range(halo.shape[1]):
            halo[m, row] = zero
        return 0

    edge[0] = zero
    edge[2 * count + 1] = zero

    lax.fori_loop(0, sweeps, clear, 0)

    barrier = pltpu.get_barrier_semaphore()
    for other in range(groups):
        @pl.when(g != other)
        def _():
            pl.semaphore_signal(barrier, inc=1, device_id={"tm": other})

    @pl.when(d > 0)
    def _():
        pl.semaphore_signal(barrier, inc=1, device_id={"space": d - 1})

    @pl.when(d < width - 1)
    def _():
        pl.semaphore_signal(barrier, inc=1, device_id={"space": d + 1})

    pl.semaphore_wait(
        barrier,
        groups - 1 + jnp.where(d > 0, 1, 0) + jnp.where(d < width - 1, 1, 0),
    )
    for load in loads:
        load.wait()

    row_id = lax.broadcasted_iota(jnp.int32, (comp, cells), 0)
    lane_id = lax.broadcasted_iota(jnp.int32, (comp, cells), 1)
    alive = live_count[0]

    def prepare(b, _):
        live = jnp.where(b < alive, 1.0, 0.0)
        mass = INVERSE_STEP * volume[pl.ds(b, 1), :]
        along = cell[pl.ds(b, 1), :]
        base = mass + jnp.sum(face[b], axis=0, keepdims=True) + 2.0 * along
        diagonal = jnp.broadcast_to(base, (comp, cells))
        for i in range(comp):
            diagonal = diagonal + jnp.where(row_id == i, jac[b, i], 0.0)
        c = live / diagonal
        rate[b] = c
        rate_cell[b] = c * along
        drift = c * mass
        rate_mass[b] = drift
        for i in range(comp):
            jac[b, i] = jnp.where(row_id == i, live - drift, 0.0) - c * jac[b, i]
        weighted[b] = zero
        return 0

    lax.fori_loop(0, nb, prepare, 0, unroll=4)

    def state_copy(to):
        return pltpu.make_async_remote_copy(
            src_ref=field.at[pl.ds(0, nb)],
            dst_ref=field.at[pl.ds(0, nb)],
            send_sem=state_send,
            recv_sem=state_recv,
            device_id={"tm": to},
        )

    @pl.when(g == groups - 1)
    def _():
        def begin(b, _):
            field[b] = jnp.where(b < alive, 1.0, 0.0) * terminal[b]
            return 0

        lax.fori_loop(0, nb, begin, 0, unroll=8)

    @pl.when(g < groups - 1)
    def _():
        state_copy(g).wait_recv()

    def halo_copy(m, side, to):
        return pltpu.make_async_remote_copy(
            src_ref=outbox.at[m, side],
            dst_ref=halo.at[m, pl.ds((1 - side) * count, count)],
            send_sem=halo_send.at[m, side],
            recv_sem=halo_recv.at[m, 1 - side],
            device_id={"space": to},
        )

    def send(m):
        @pl.when(d > 0)
        def _():
            halo_copy(m, 0, d - 1).start()

        @pl.when(d < width - 1)
        def _():
            halo_copy(m, 1, d + 1).start()

    def receive(m):
        @pl.when(d > 0)
        def _():
            halo_copy(m, 1, d - 1).wait_recv()

        @pl.when(d < width - 1)
        def _():
            halo_copy(m, 0, d + 1).wait_recv()

    def remote(b):
        value = None
        for k in range(nei):
            slot = jnp.maximum(nbr[b, k], nb - 1) - (nb - 1)
            term = face[b, pl.ds(k, 1), :] * edge[slot]
            value = term if value is None else value + term
        return part[b] + rate[b] * value

    for side in range(2):
        for s in range(count):
            outbox[0, side, s] = field[send_blocks[0, side, s]]
    send(0)

    def sweep(m, n):
        def local(b0, _):
            for u in range(UNROLL):
                b = b0 * UNROLL + u
                x = field[b]
                left = jnp.where(lane_id == 0, 0.0, pltpu.roll(x, 1, 1))
                right = jnp.where(lane_id == cells - 1, 0.0, pltpu.roll(x, cells - 1, 1))
                value = rhs[b] + rate_cell[b] * (left + right)
                for i in range(comp):
                    value = value + jac[b, i] * field[b, pl.ds(i, 1), :]
                near = None
                for k in range(nei):
                    term = face[b, pl.ds(k, 1), :] * field[jnp.minimum(nbr[b, k], nb)]
                    near = term if near is None else near + term
                part[b] = value + rate[b] * near
            return 0

        lax.fori_loop(0, nb // UNROLL, local, 0)
        receive(m)
        for row in range(2 * count):
            edge[1 + row] = halo[m, row]

        @pl.when(m + 1 < sweeps)
        def _():
            for side in range(2):
                for s in range(count):
                    outbox[m + 1, side, s] = remote(send_blocks[0, side, s])
            send(m + 1)

        def bulk(b0, _):
            for u in range(UNROLL):
                b = b0 * UNROLL + u
                field[b] = remote(b)
            return 0

        lax.fori_loop(0, nb // UNROLL, bulk, 0)

    def level_copy(n):
        return pltpu.make_async_copy(levels.at[n], adjoint_hbm.at[n], store_sem.at[n])

    def level(t, _):
        n = steps - 1 - t

        def start(b0, _):
            for u in range(UNROLL):
                b = b0 * UNROLL + u
                rhs[b] = rate[b] * source[n, b] + rate_mass[b] * field[b]
            return 0

        lax.fori_loop(0, nb // UNROLL, start, 0)

        def inner(it, _):
            sweep(t * ITERS + it, n)
            return 0

        lax.fori_loop(0, ITERS, inner, 0)

        @pl.when((t == steps - 1) & (g > 0))
        def _():
            state_copy(g - 1).start()

        weight = weights[n]

        def finish(b0, _):
            for u in range(UNROLL):
                b = b0 * UNROLL + u
                x = field[b]
                levels[n, b] = x
                weighted[b] = weighted[b] + weight * x
            return 0

        lax.fori_loop(0, nb // UNROLL, finish, 0)
        level_copy(n).start()
        return 0

    lax.fori_loop(0, steps, level, 0)

    summed = jnp.sum(weighted[...] * shape[...], axis=1)
    mine = lax.dot_general(
        jnp.ones((8, cells), jnp.float32),
        summed,
        (((1,), (1,)), ((), ())),
        precision=lax.Precision.HIGHEST,
        preferred_element_type=jnp.float32,
    )

    def acc_copy(to):
        return pltpu.make_async_remote_copy(
            src_ref=acc_out, dst_ref=acc_in, send_sem=acc_send, recv_sem=acc_recv,
            device_id={"tm": to},
        )

    def total_copy(to):
        return pltpu.make_async_remote_copy(
            src_ref=acc_out, dst_ref=total, send_sem=total_send.at[to], recv_sem=total_recv,
            device_id={"tm": to},
        )

    @pl.when(g == groups - 1)
    def _():
        acc_out[...] = mine

    @pl.when(g < groups - 1)
    def _():
        acc_copy(g).wait_recv()
        acc_out[...] = mine + acc_in[...]

    @pl.when(g > 0)
    def _():
        acc_copy(g - 1).start()
        total_copy(g).wait_recv()
        sens_ref[...] = total[0:1, :]

    @pl.when(g == 0)
    def _():
        for other in range(1, groups):
            total_copy(other).start()
        sens_ref[...] = acc_out[0:1, :]
        for other in range(1, groups):
            total_copy(other).wait_send()

    @pl.when(g > 0)
    def _():
        acc_copy(g - 1).wait_send()
        state_copy(g - 1).wait_send()

    def drain(m, _):
        @pl.when(d > 0)
        def _():
            halo_copy(m, 0, d - 1).wait_send()

        @pl.when(d < width - 1)
        def _():
            halo_copy(m, 1, d + 1).wait_send()

        return 0

    lax.fori_loop(0, sweeps, drain, 0)
    for n in range(steps):
        level_copy(n).wait()


def per_device(groups, width, *args):
    (source, terminal, jacobian, face_coef, cell_coef, neighbours, send_blocks,
     live_count, volume, shape_field, weights) = args
    steps, nb, comp, cells = source.shape
    nei = face_coef.shape[1]
    count = send_blocks.shape[2]
    sweeps = steps * ITERS
    f32 = jnp.float32
    hbm = pl.BlockSpec(memory_space=pl.ANY)
    smem = pl.BlockSpec(memory_space=pltpu.SMEM)
    vmem = pltpu.VMEM
    dma = pltpu.SemaphoreType.DMA
    block = (nb, comp, cells)
    adjoint, sens = pl.pallas_call(
        functools.partial(kernel, groups, width),
        out_shape=(
            jax.ShapeDtypeStruct(source.shape, f32),
            jax.ShapeDtypeStruct((1, nb), f32),
        ),
        in_specs=[hbm, hbm, hbm, hbm, hbm, smem, smem, smem, hbm, hbm, smem],
        out_specs=(hbm, pl.BlockSpec(memory_space=pltpu.VMEM)),
        scratch_shapes=[
            vmem(source.shape, f32),
            vmem(block, f32),
            vmem(jacobian.shape[1:], f32),
            vmem(face_coef.shape, f32),
            vmem(cell_coef.shape, f32),
            vmem(volume.shape, f32),
            vmem(block, f32),
            vmem((nb + 1, comp, cells), f32),
            vmem(block, f32),
            vmem(block, f32),
            vmem(block, f32),
            vmem(block, f32),
            vmem(block, f32),
            vmem(source.shape, f32),
            vmem(block, f32),
            vmem((sweeps, 2 * count, comp, cells), f32),
            vmem((2 * count + 2, comp, cells), f32),
            vmem((sweeps, 2, count, comp, cells), f32),
            vmem((8, nb), f32),
            vmem((8, nb), f32),
            vmem((8, nb), f32),
            dma((7,)),
            dma((steps,)),
            dma((sweeps, 2)),
            dma((sweeps, 2)),
            dma,
            dma,
            dma,
            dma,
            dma((groups,)),
            dma,
        ],
        compiler_params=pltpu.CompilerParams(collective_id=0, has_side_effects=True),
    )(*args)
    return adjoint, sens.reshape(nb)


def solution(mesh):
    sizes = dict(mesh.shape)
    return jax.shard_map(
        functools.partial(per_device, sizes["tm"], sizes["space"]),
        mesh=mesh,
        in_specs=(
            P("tm", "space", None, None),
            P("space", None, None),
            P("tm", "space", None, None, None),
            P("space", None, None),
            P("space", None),
            P("space", None),
            P("space", None, None),
            P("space"),
            P("space", None),
            P("space", None, None),
            P("tm"),
        ),
        out_specs=(P("tm", "space", None, None), P("space")),
        check_vma=False,
    )
```

```python
import functools

import jax
import jax.numpy as jnp
from jax import lax
from jax.experimental import pallas as pl
from jax.experimental.pallas import tpu as pltpu
from jax.sharding import PartitionSpec as P

ITERS = 3
INVERSE_STEP = 6.0
TILE = 16
HIGHEST = lax.Precision.HIGHEST


def split(x):
    high = x.astype(jnp.bfloat16)
    return high, (x - high.astype(jnp.float32)).astype(jnp.bfloat16)


def matmul(a, b, precision=None):
    return jnp.dot(a, b, precision=precision, preferred_element_type=jnp.float32)


def kernel(
    groups,
    width,
    source_hbm,
    terminal_hbm,
    jac_hbm,
    face_hbm,
    cell_hbm,
    nbr_hbm,
    send_blocks,
    live_count,
    volume_hbm,
    shape_hbm,
    weights,
    adjoint_hbm,
    sens_ref,
    source,
    terminal,
    jac,
    face,
    cell,
    nbr,
    volume,
    shape,
    field,
    part,
    rate,
    rate_mass,
    cell_left,
    cell_right,
    rhs,
    levels,
    weighted,
    near_pick,
    far_pick,
    field_terms,
    part_terms,
    halo_terms,
    near,
    far,
    select,
    select_terms,
    edge_pick,
    edge_face,
    edge_rate,
    edge_part,
    halo,
    outbox,
    acc_in,
    acc_out,
    total,
    load_sem,
    store_sem,
    halo_send,
    halo_recv,
    state_send,
    state_recv,
    acc_send,
    acc_recv,
    total_send,
    total_recv,
):
    g = lax.axis_index("tm")
    d = lax.axis_index("space")
    steps, comp, nb, cells = source.shape
    nei = face.shape[0]
    count = outbox.shape[3]
    sweeps = steps * ITERS
    tiles = nb // TILE
    edges = 2 * count

    loads = [
        pltpu.make_async_copy(nbr_hbm, nbr, load_sem.at[0]),
        pltpu.make_async_copy(face_hbm, face, load_sem.at[1]),
        pltpu.make_async_copy(cell_hbm, cell, load_sem.at[2]),
        pltpu.make_async_copy(volume_hbm, volume, load_sem.at[3]),
        pltpu.make_async_copy(jac_hbm.at[0], jac, load_sem.at[4]),
        pltpu.make_async_copy(terminal_hbm, terminal, load_sem.at[5]),
        pltpu.make_async_copy(source_hbm, source, load_sem.at[6]),
        pltpu.make_async_copy(shape_hbm, shape, load_sem.at[7]),
    ]
    for load in loads:
        load.start()

    @pl.when((d == 0) | (d == width - 1))
    def _():
        halo[...] = jnp.zeros_like(halo)

    barrier = pltpu.get_barrier_semaphore()
    for other in range(groups):
        @pl.when(g != other)
        def _():
            pl.semaphore_signal(barrier, inc=1, device_id={"tm": other})

    @pl.when(d > 0)
    def _():
        pl.semaphore_signal(barrier, inc=1, device_id={"space": d - 1})

    @pl.when(d < width - 1)
    def _():
        pl.semaphore_signal(barrier, inc=1, device_id={"space": d + 1})

    halo_terms[...] = jnp.zeros_like(halo_terms)
    lane = lax.broadcasted_iota(jnp.int32, (1, nb), 1)
    for side in range(2):
        for s in range(count):
            row = side * count + s
            select[pl.ds(row, 1), :] = jnp.where(lane == send_blocks[0, side, s], 1.0, 0.0)
    chosen = select[...]
    chosen_low = chosen.astype(jnp.bfloat16)
    select_terms[:, :nb] = chosen_low
    select_terms[:, nb:] = chosen_low

    loads[0].wait()
    listed = nbr[...].astype(jnp.float32)
    listed = jnp.concatenate([listed, jnp.zeros((nb - nei, nb), jnp.float32)], axis=0).T
    wide = lax.broadcasted_iota(jnp.int32, (nb, nb), 1).astype(jnp.float32)
    for k in range(nei):
        column = jnp.broadcast_to(listed[:, k : k + 1], (nb, nb))
        pick = jnp.where(column == wide, 1.0, 0.0).astype(jnp.bfloat16)
        near_pick[pl.ds(k * nb, nb), :nb] = pick
        near_pick[pl.ds(k * nb, nb), nb:] = pick
        outer = column - nb
        hit = (outer == wide) | (outer + edges == wide)
        inside = (outer >= 0) & (outer < edges)
        pick = jnp.where(hit & inside, 1.0, 0.0).astype(jnp.bfloat16)
        far_pick[pl.ds(k * nb, nb), :] = pick
        edge_pick[pl.ds(k * edges, edges), :] = matmul(chosen_low, pick).astype(jnp.bfloat16)

    for load in loads[1:5]:
        load.wait()
    alive = live_count[0]
    row_id = lax.broadcasted_iota(jnp.int32, (TILE, cells), 0)
    lane_id = lax.broadcasted_iota(jnp.int32, (TILE, cells), 1)

    def live_of(t):
        return jnp.where(row_id + t * TILE < alive, 1.0, 0.0)

    def prepare(t, _):
        r = pl.ds(pl.multiple_of(t * TILE, TILE), TILE)
        live = live_of(t)
        mass = INVERSE_STEP * volume[r, :]
        along = cell[r, :]
        base = mass + 2.0 * along
        for k in range(nei):
            base = base + face[k, r, :]
        cell_left[r, :] = jnp.where(lane_id == 0, 0.0, along)
        cell_right[r, :] = jnp.where(lane_id == cells - 1, 0.0, along)
        for j in range(comp):
            c = live / (base + jac[j, j, r, :])
            rate[j, r, :] = c
            drift = c * mass
            rate_mass[j, r, :] = drift
            for i in range(comp):
                entry = -c * jac[i, j, r, :]
                jac[i, j, r, :] = entry + (live - drift) if i == j else entry
            weighted[j, r, :] = jnp.zeros((TILE, cells), jnp.float32)
        return 0

    lax.fori_loop(0, tiles, prepare, 0)
    for k in range(nei):
        edge_face[k] = matmul(chosen, face[k], HIGHEST)
    for j in range(comp):
        edge_rate[j] = matmul(chosen, rate[j], HIGHEST)

    for load in loads[5:]:
        load.wait()
    pl.semaphore_wait(
        barrier,
        groups - 1 + jnp.where(d > 0, 1, 0) + jnp.where(d < width - 1, 1, 0),
    )

    def lanes(j):
        return slice(j * cells, (j + 1) * cells)

    def put_terms(ref, t, j, x):
        high, low = split(x)
        ref[pl.ds(pl.multiple_of(t * TILE, TILE), TILE), lanes(j)] = high
        ref[pl.ds(pl.multiple_of(nb + t * TILE, TILE), TILE), lanes(j)] = low

    def state_copy(to):
        return pltpu.make_async_remote_copy(
            src_ref=field, dst_ref=field, send_sem=state_send, recv_sem=state_recv,
            device_id={"tm": to},
        )

    @pl.when(g == groups - 1)
    def _():
        def begin(t, _):
            r = pl.ds(pl.multiple_of(t * TILE, TILE), TILE)
            for j in range(comp):
                field[j, r, :] = live_of(t) * terminal[j, r, :]
            return 0

        lax.fori_loop(0, tiles, begin, 0)

    @pl.when(g < groups - 1)
    def _():
        state_copy(g).wait_recv()

    def begin_terms(t, _):
        r = pl.ds(pl.multiple_of(t * TILE, TILE), TILE)
        for j in range(comp):
            put_terms(field_terms, t, j, field[j, r, :])
        return 0

    lax.fori_loop(0, tiles, begin_terms, 0)

    def halo_copy(m, side, to):
        return pltpu.make_async_remote_copy(
            src_ref=outbox.at[m, side],
            dst_ref=halo.at[m, 1 - side],
            send_sem=halo_send.at[m, side],
            recv_sem=halo_recv.at[m, 1 - side],
            device_id={"space": to},
        )

    def send(m):
        @pl.when(d > 0)
        def _():
            halo_copy(m, 0, d - 1).start()

        @pl.when(d < width - 1)
        def _():
            halo_copy(m, 1, d + 1).start()

    def receive(m):
        @pl.when(d > 0)
        def _():
            halo_copy(m, 1, d - 1).wait_recv()

        @pl.when(d < width - 1)
        def _():
            halo_copy(m, 0, d + 1).wait_recv()

    first_out = matmul(select_terms[...], field_terms[...])
    for side in range(2):
        for j in range(comp):
            outbox[0, side, j] = first_out[side * count : (side + 1) * count, lanes(j)]
    send(0)

    def sweep(m):
        near[...] = matmul(near_pick[...], field_terms[...])

        def local(t, _):
            r = pl.ds(pl.multiple_of(t * TILE, TILE), TILE)
            x = [field[i, r, :] for i in range(comp)]
            left = cell_left[r, :]
            right = cell_right[r, :]
            for j in range(comp):
                value = left * pltpu.roll(x[j], 1, 1) + right * pltpu.roll(x[j], cells - 1, 1)
                for k in range(nei):
                    q = pl.ds(pl.multiple_of(k * nb + t * TILE, TILE), TILE)
                    value = value + face[k, r, :] * near[q, lanes(j)]
                value = rhs[j, r, :] + rate[j, r, :] * value
                for i in range(comp):
                    value = value + jac[i, j, r, :] * x[i]
                part[j, r, :] = value
                put_terms(part_terms, t, j, value)
            return 0

        lax.fori_loop(0, tiles, local, 0)
        edge_part[...] = matmul(select_terms[...], part_terms[...])
        receive(m)
        for side in range(2):
            for j in range(comp):
                high, low = split(halo[m, side, j])
                halo_terms[side * count : (side + 1) * count, lanes(j)] = high
                halo_terms[edges + side * count : edges + (side + 1) * count, lanes(j)] = low

        @pl.when(m + 1 < sweeps)
        def _():
            arrived = matmul(edge_pick[...], halo_terms[...])
            for side in range(2):
                rows = slice(side * count, (side + 1) * count)
                for j in range(comp):
                    value = None
                    for k in range(nei):
                        q = slice(k * edges + side * count, k * edges + (side + 1) * count)
                        term = edge_face[k, rows, :] * arrived[q, lanes(j)]
                        value = term if value is None else value + term
                    outbox[m + 1, side, j] = edge_part[rows, lanes(j)] + edge_rate[j, rows, :] * value
            send(m + 1)

        far[...] = matmul(far_pick[...], halo_terms[...])

        def bulk(t, _):
            r = pl.ds(pl.multiple_of(t * TILE, TILE), TILE)
            for j in range(comp):
                value = None
                for k in range(nei):
                    q = pl.ds(pl.multiple_of(k * nb + t * TILE, TILE), TILE)
                    term = face[k, r, :] * far[q, lanes(j)]
                    value = term if value is None else value + term
                value = part[j, r, :] + rate[j, r, :] * value
                field[j, r, :] = value
                put_terms(field_terms, t, j, value)
            return 0

        lax.fori_loop(0, tiles, bulk, 0)

    def level_copy(n):
        return pltpu.make_async_copy(levels.at[n], adjoint_hbm.at[n], store_sem.at[n])

    def level(step, _):
        n = steps - 1 - step

        def start(t, _):
            r = pl.ds(pl.multiple_of(t * TILE, TILE), TILE)
            for j in range(comp):
                rhs[j, r, :] = rate[j, r, :] * source[n, j, r, :] + rate_mass[j, r, :] * field[j, r, :]
            return 0

        lax.fori_loop(0, tiles, start, 0)

        def inner(it, _):
            sweep(step * ITERS + it)
            return 0

        lax.fori_loop(0, ITERS, inner, 0)

        @pl.when((step == steps - 1) & (g > 0))
        def _():
            state_copy(g - 1).start()

        weight = weights[n]

        def finish(t, _):
            r = pl.ds(pl.multiple_of(t * TILE, TILE), TILE)
            for j in range(comp):
                x = field[j, r, :]
                levels[n, j, r, :] = x
                weighted[j, r, :] = weighted[j, r, :] + weight * x
            return 0

        lax.fori_loop(0, tiles, finish, 0)
        level_copy(n).start()
        return 0

    lax.fori_loop(0, steps, level, 0)

    summed = jnp.zeros((nb, cells), jnp.float32)
    for j in range(comp):
        summed = summed + weighted[j] * shape[j]

    mine = lax.dot_general(
        jnp.ones((8, cells), jnp.float32),
        summed,
        (((1,), (1,)), ((), ())),
        precision=lax.Precision.HIGHEST,
        preferred_element_type=jnp.float32,
    )

    def acc_copy(to):
        return pltpu.make_async_remote_copy(
            src_ref=acc_out, dst_ref=acc_in, send_sem=acc_send, recv_sem=acc_recv,
            device_id={"tm": to},
        )

    def total_copy(to):
        return pltpu.make_async_remote_copy(
            src_ref=acc_out, dst_ref=total, send_sem=total_send.at[to], recv_sem=total_recv,
            device_id={"tm": to},
        )

    @pl.when(g == groups - 1)
    def _():
        acc_out[...] = mine

    @pl.when(g < groups - 1)
    def _():
        acc_copy(g).wait_recv()
        acc_out[...] = mine + acc_in[...]

    @pl.when(g > 0)
    def _():
        acc_copy(g - 1).start()
        total_copy(g).wait_recv()
        sens_ref[...] = total[0:1, :]

    @pl.when(g == 0)
    def _():
        for other in range(1, groups):
            total_copy(other).start()
        sens_ref[...] = acc_out[0:1, :]
        for other in range(1, groups):
            total_copy(other).wait_send()

    @pl.when(g > 0)
    def _():
        acc_copy(g - 1).wait_send()
        state_copy(g - 1).wait_send()

    def drain(m, _):
        @pl.when(d > 0)
        def _():
            halo_copy(m, 0, d - 1).wait_send()

        @pl.when(d < width - 1)
        def _():
            halo_copy(m, 1, d + 1).wait_send()

        return 0

    lax.fori_loop(0, sweeps, drain, 0)
    for n in range(steps):
        level_copy(n).wait()


def per_device(groups, width, *args):
    (source, terminal, jacobian, face_coef, cell_coef, neighbours, send_blocks,
     live_count, volume, shape_field, weights) = args
    steps, nb, comp, cells = source.shape
    nei = face_coef.shape[1]
    count = send_blocks.shape[2]
    edges = 2 * count
    sweeps = steps * ITERS
    f32 = jnp.float32
    bf16 = jnp.bfloat16
    hbm = pl.BlockSpec(memory_space=pltpu.MemorySpace.HBM)
    smem = pl.BlockSpec(memory_space=pltpu.SMEM)
    vmem = pltpu.VMEM
    dma = pltpu.SemaphoreType.DMA
    block = (comp, nb, cells)
    flat = comp * cells
    adjoint, sens = pl.pallas_call(
        functools.partial(kernel, groups, width),
        out_shape=(
            jax.ShapeDtypeStruct((steps, comp, nb, cells), f32),
            jax.ShapeDtypeStruct((1, nb), f32),
        ),
        in_specs=[hbm, hbm, hbm, hbm, hbm, hbm, smem, smem, hbm, hbm, smem],
        out_specs=(hbm, pl.BlockSpec(memory_space=pltpu.VMEM)),
        scratch_shapes=[
            vmem((steps, comp, nb, cells), f32),
            vmem(block, f32),
            vmem((comp, comp, nb, cells), f32),
            vmem((nei, nb, cells), f32),
            vmem((nb, cells), f32),
            vmem((nei, nb), jnp.int32),
            vmem((nb, cells), f32),
            vmem(block, f32),
            vmem(block, f32),
            vmem(block, f32),
            vmem(block, f32),
            vmem(block, f32),
            vmem((nb, cells), f32),
            vmem((nb, cells), f32),
            vmem(block, f32),
            vmem((steps, comp, nb, cells), f32),
            vmem(block, f32),
            vmem((nei * nb, 2 * nb), bf16),
            vmem((nei * nb, nb), bf16),
            vmem((2 * nb, flat), bf16),
            vmem((2 * nb, flat), bf16),
            vmem((nb, flat), bf16),
            vmem((nei * nb, flat), f32),
            vmem((nei * nb, flat), f32),
            vmem((edges, nb), f32),
            vmem((edges, 2 * nb), bf16),
            vmem((nei * edges, nb), bf16),
            vmem((nei, edges, cells), f32),
            vmem((comp, edges, cells), f32),
            vmem((edges, flat), f32),
            vmem((sweeps, 2, comp, count, cells), f32),
            vmem((sweeps, 2, comp, count, cells), f32),
            vmem((8, nb), f32),
            vmem((8, nb), f32),
            vmem((8, nb), f32),
            dma((8,)),
            dma((steps,)),
            dma((sweeps, 2)),
            dma((sweeps, 2)),
            dma,
            dma,
            dma,
            dma,
            dma((groups,)),
            dma,
        ],
        compiler_params=pltpu.CompilerParams(collective_id=0, has_side_effects=True),
    )(
        source.transpose(0, 2, 1, 3),
        terminal.transpose(1, 0, 2),
        jacobian.transpose(0, 2, 3, 1, 4),
        face_coef.transpose(1, 0, 2),
        cell_coef,
        neighbours.T,
        send_blocks,
        live_count,
        volume,
        shape_field.transpose(1, 0, 2),
        weights,
    )
    return adjoint.transpose(0, 2, 1, 3), sens.reshape(nb)


def solution(mesh):
    sizes = dict(mesh.shape)
    return jax.shard_map(
        functools.partial(per_device, sizes["tm"], sizes["space"]),
        mesh=mesh,
        in_specs=(
            P("tm", "space", None, None),
            P("space", None, None),
            P("tm", "space", None, None, None),
            P("space", None, None),
            P("space", None),
            P("space", None),
            P("space", None, None),
            P("space"),
            P("space", None),
            P("space", None, None),
            P("tm"),
        ),
        out_specs=(P("tm", "space", None, None), P("space")),
        check_vma=False,
    )
```

```python
import functools

import jax
import jax.numpy as jnp
from jax import lax
from jax.experimental import pallas as pl
from jax.experimental.pallas import tpu as pltpu
from jax.sharding import PartitionSpec as P

ITERS = 3
INVERSE_STEP = 6.0
TILE = 16
HIGHEST = lax.Precision.HIGHEST


def rows_at(start):
    return pl.ds(start if isinstance(start, int) else pl.multiple_of(start, TILE), TILE)


def split(x):
    high = x.astype(jnp.bfloat16)
    return high, (x - high.astype(jnp.float32)).astype(jnp.bfloat16)


def matmul(a, b, precision=None):
    return jnp.dot(a, b, precision=precision, preferred_element_type=jnp.float32)


def kernel(
    groups,
    width,
    source_hbm,
    terminal_hbm,
    jac_hbm,
    face_hbm,
    cell_hbm,
    nbr_hbm,
    send_blocks,
    live_count,
    volume_hbm,
    shape_hbm,
    weights,
    adjoint_hbm,
    sens_ref,
    source,
    terminal,
    jac,
    face,
    cell,
    nbr,
    volume,
    shape,
    field,
    part,
    rate,
    rate_mass,
    cell_left,
    cell_right,
    rhs,
    levels,
    weighted,
    near_pick,
    far_pick,
    field_terms,
    part_terms,
    halo_terms,
    near,
    far,
    select,
    select_terms,
    edge_pick,
    edge_face,
    edge_rate,
    edge_part,
    halo,
    outbox,
    acc_in,
    acc_out,
    total,
    load_sem,
    store_sem,
    halo_send,
    halo_recv,
    state_send,
    state_recv,
    acc_send,
    acc_recv,
    total_send,
    total_recv,
):
    g = lax.axis_index("tm")
    d = lax.axis_index("space")
    steps, comp, nb, cells = source.shape
    nei = face.shape[0]
    count = outbox.shape[3]
    sweeps = steps * ITERS
    tiles = nb // TILE
    edges = 2 * count

    loads = [
        pltpu.make_async_copy(nbr_hbm, nbr, load_sem.at[0]),
        pltpu.make_async_copy(face_hbm, face, load_sem.at[1]),
        pltpu.make_async_copy(cell_hbm, cell, load_sem.at[2]),
        pltpu.make_async_copy(volume_hbm, volume, load_sem.at[3]),
        pltpu.make_async_copy(jac_hbm.at[0], jac, load_sem.at[4]),
        pltpu.make_async_copy(terminal_hbm, terminal, load_sem.at[5]),
        pltpu.make_async_copy(source_hbm, source, load_sem.at[6]),
        pltpu.make_async_copy(shape_hbm, shape, load_sem.at[7]),
    ]
    for load in loads:
        load.start()

    @pl.when((d == 0) | (d == width - 1))
    def _():
        halo[...] = jnp.zeros_like(halo)

    barrier = pltpu.get_barrier_semaphore()
    for other in range(groups):
        @pl.when(g != other)
        def _():
            pl.semaphore_signal(barrier, inc=1, device_id={"tm": other})

    @pl.when(d > 0)
    def _():
        pl.semaphore_signal(barrier, inc=1, device_id={"space": d - 1})

    @pl.when(d < width - 1)
    def _():
        pl.semaphore_signal(barrier, inc=1, device_id={"space": d + 1})

    halo_terms[...] = jnp.zeros_like(halo_terms)
    lane = lax.broadcasted_iota(jnp.int32, (1, nb), 1)
    for side in range(2):
        for s in range(count):
            row = side * count + s
            select[pl.ds(row, 1), :] = jnp.where(lane == send_blocks[0, side, s], 1.0, 0.0)
    chosen = select[...]
    chosen_low = chosen.astype(jnp.bfloat16)
    select_terms[:, :nb] = chosen_low
    select_terms[:, nb:] = chosen_low

    loads[0].wait()
    listed = nbr[...].astype(jnp.float32)
    listed = jnp.concatenate([listed, jnp.zeros((nb - nei, nb), jnp.float32)], axis=0).T
    wide = lax.broadcasted_iota(jnp.int32, (nb, nb), 1).astype(jnp.float32)
    for k in range(nei):
        column = jnp.broadcast_to(listed[:, k : k + 1], (nb, nb))
        pick = jnp.where(column == wide, 1.0, 0.0).astype(jnp.bfloat16)
        near_pick[pl.ds(k * nb, nb), :nb] = pick
        near_pick[pl.ds(k * nb, nb), nb:] = pick
        outer = column - nb
        hit = (outer == wide) | (outer + edges == wide)
        inside = (outer >= 0) & (outer < edges)
        pick = jnp.where(hit & inside, 1.0, 0.0).astype(jnp.bfloat16)
        far_pick[pl.ds(k * nb, nb), :] = pick
        edge_pick[pl.ds(k * edges, edges), :] = matmul(chosen_low, pick).astype(jnp.bfloat16)

    for load in loads[1:5]:
        load.wait()
    alive = live_count[0]
    row_id = lax.broadcasted_iota(jnp.int32, (TILE, cells), 0)
    lane_id = lax.broadcasted_iota(jnp.int32, (TILE, cells), 1)

    def live_of(t):
        return jnp.where(row_id + t * TILE < alive, 1.0, 0.0)

    def prepare(t, _):
        r = rows_at(t * TILE)
        live = live_of(t)
        mass = INVERSE_STEP * volume[r, :]
        along = cell[r, :]
        base = mass + 2.0 * along
        for k in range(nei):
            base = base + face[k, r, :]
        cell_left[r, :] = jnp.where(lane_id == 0, 0.0, along)
        cell_right[r, :] = jnp.where(lane_id == cells - 1, 0.0, along)
        for j in range(comp):
            c = live / (base + jac[j, j, r, :])
            rate[j, r, :] = c
            drift = c * mass
            rate_mass[j, r, :] = drift
            for i in range(comp):
                entry = -c * jac[i, j, r, :]
                jac[i, j, r, :] = entry + (live - drift) if i == j else entry
            weighted[j, r, :] = jnp.zeros((TILE, cells), jnp.float32)
        return 0

    lax.fori_loop(0, tiles, prepare, 0)
    for k in range(nei):
        edge_face[k] = matmul(chosen, face[k], HIGHEST)
    for j in range(comp):
        edge_rate[j] = matmul(chosen, rate[j], HIGHEST)

    for load in loads[5:]:
        load.wait()
    pl.semaphore_wait(
        barrier,
        groups - 1 + jnp.where(d > 0, 1, 0) + jnp.where(d < width - 1, 1, 0),
    )

    def lanes(j):
        return slice(j * cells, (j + 1) * cells)

    def put_terms(ref, t, j, x):
        high, low = split(x)
        ref[rows_at(t * TILE), lanes(j)] = high
        ref[rows_at(nb + t * TILE), lanes(j)] = low

    def state_copy(to):
        return pltpu.make_async_remote_copy(
            src_ref=field, dst_ref=field, send_sem=state_send, recv_sem=state_recv,
            device_id={"tm": to},
        )

    @pl.when(g == groups - 1)
    def _():
        def begin(t, _):
            r = rows_at(t * TILE)
            for j in range(comp):
                field[j, r, :] = live_of(t) * terminal[j, r, :]
            return 0

        lax.fori_loop(0, tiles, begin, 0)

    @pl.when(g < groups - 1)
    def _():
        state_copy(g).wait_recv()

    def begin_terms(t, _):
        r = rows_at(t * TILE)
        for j in range(comp):
            put_terms(field_terms, t, j, field[j, r, :])
        return 0

    lax.fori_loop(0, tiles, begin_terms, 0)

    def halo_copy(m, side, to):
        return pltpu.make_async_remote_copy(
            src_ref=outbox.at[m, side],
            dst_ref=halo.at[m, 1 - side],
            send_sem=halo_send.at[m, side],
            recv_sem=halo_recv.at[m, 1 - side],
            device_id={"space": to},
        )

    def send(m):
        @pl.when(d > 0)
        def _():
            halo_copy(m, 0, d - 1).start()

        @pl.when(d < width - 1)
        def _():
            halo_copy(m, 1, d + 1).start()

    def receive(m):
        @pl.when(d > 0)
        def _():
            halo_copy(m, 1, d - 1).wait_recv()

        @pl.when(d < width - 1)
        def _():
            halo_copy(m, 0, d + 1).wait_recv()

    first_out = matmul(select_terms[...], field_terms[...])
    for side in range(2):
        for j in range(comp):
            outbox[0, side, j] = first_out[side * count : (side + 1) * count, lanes(j)]
    send(0)

    def sweep(m):
        near[...] = matmul(near_pick[...], field_terms[...])

        def local(t, _):
            r = rows_at(t * TILE)
            x = [field[i, r, :] for i in range(comp)]
            left = cell_left[r, :]
            right = cell_right[r, :]
            for j in range(comp):
                value = left * pltpu.roll(x[j], 1, 1) + right * pltpu.roll(x[j], cells - 1, 1)
                for k in range(nei):
                    q = rows_at(k * nb + t * TILE)
                    value = value + face[k, r, :] * near[q, lanes(j)]
                value = rhs[j, r, :] + rate[j, r, :] * value
                for i in range(comp):
                    value = value + jac[i, j, r, :] * x[i]
                part[j, r, :] = value
                put_terms(part_terms, t, j, value)
            return 0

        for t in range(tiles):
            local(t, 0)
        edge_part[...] = matmul(select_terms[...], part_terms[...])
        receive(m)
        for side in range(2):
            for j in range(comp):
                high, low = split(halo[m, side, j])
                halo_terms[side * count : (side + 1) * count, lanes(j)] = high
                halo_terms[edges + side * count : edges + (side + 1) * count, lanes(j)] = low

        @pl.when(m + 1 < sweeps)
        def _():
            arrived = matmul(edge_pick[...], halo_terms[...])
            for side in range(2):
                rows = slice(side * count, (side + 1) * count)
                for j in range(comp):
                    value = None
                    for k in range(nei):
                        q = slice(k * edges + side * count, k * edges + (side + 1) * count)
                        term = edge_face[k, rows, :] * arrived[q, lanes(j)]
                        value = term if value is None else value + term
                    outbox[m + 1, side, j] = edge_part[rows, lanes(j)] + edge_rate[j, rows, :] * value
            send(m + 1)

        far[...] = matmul(far_pick[...], halo_terms[...])

        def bulk(t, _):
            r = rows_at(t * TILE)
            for j in range(comp):
                value = None
                for k in range(nei):
                    q = rows_at(k * nb + t * TILE)
                    term = face[k, r, :] * far[q, lanes(j)]
                    value = term if value is None else value + term
                value = part[j, r, :] + rate[j, r, :] * value
                field[j, r, :] = value
                put_terms(field_terms, t, j, value)
            return 0

        for t in range(tiles):
            bulk(t, 0)

    def level_copy(n):
        return pltpu.make_async_copy(levels.at[n], adjoint_hbm.at[n], store_sem.at[n])

    def level(step, _):
        n = steps - 1 - step

        def start(t, _):
            r = rows_at(t * TILE)
            for j in range(comp):
                rhs[j, r, :] = rate[j, r, :] * source[n, j, r, :] + rate_mass[j, r, :] * field[j, r, :]
            return 0

        lax.fori_loop(0, tiles, start, 0)

        def inner(it, _):
            sweep(step * ITERS + it)
            return 0

        lax.fori_loop(0, ITERS, inner, 0)

        @pl.when((step == steps - 1) & (g > 0))
        def _():
            state_copy(g - 1).start()

        weight = weights[n]

        def finish(t, _):
            r = rows_at(t * TILE)
            for j in range(comp):
                x = field[j, r, :]
                levels[n, j, r, :] = x
                weighted[j, r, :] = weighted[j, r, :] + weight * x
            return 0

        lax.fori_loop(0, tiles, finish, 0)
        level_copy(n).start()
        return 0

    lax.fori_loop(0, steps, level, 0)

    summed = jnp.zeros((nb, cells), jnp.float32)
    for j in range(comp):
        summed = summed + weighted[j] * shape[j]

    mine = lax.dot_general(
        jnp.ones((8, cells), jnp.float32),
        summed,
        (((1,), (1,)), ((), ())),
        precision=lax.Precision.HIGHEST,
        preferred_element_type=jnp.float32,
    )

    def acc_copy(to):
        return pltpu.make_async_remote_copy(
            src_ref=acc_out, dst_ref=acc_in, send_sem=acc_send, recv_sem=acc_recv,
            device_id={"tm": to},
        )

    def total_copy(to):
        return pltpu.make_async_remote_copy(
            src_ref=acc_out, dst_ref=total, send_sem=total_send.at[to], recv_sem=total_recv,
            device_id={"tm": to},
        )

    @pl.when(g == groups - 1)
    def _():
        acc_out[...] = mine

    @pl.when(g < groups - 1)
    def _():
        acc_copy(g).wait_recv()
        acc_out[...] = mine + acc_in[...]

    @pl.when(g > 0)
    def _():
        acc_copy(g - 1).start()
        total_copy(g).wait_recv()
        sens_ref[...] = total[0:1, :]

    @pl.when(g == 0)
    def _():
        for other in range(1, groups):
            total_copy(other).start()
        sens_ref[...] = acc_out[0:1, :]
        for other in range(1, groups):
            total_copy(other).wait_send()

    @pl.when(g > 0)
    def _():
        acc_copy(g - 1).wait_send()
        state_copy(g - 1).wait_send()

    def drain(m, _):
        @pl.when(d > 0)
        def _():
            halo_copy(m, 0, d - 1).wait_send()

        @pl.when(d < width - 1)
        def _():
            halo_copy(m, 1, d + 1).wait_send()

        return 0

    lax.fori_loop(0, sweeps, drain, 0)
    for n in range(steps):
        level_copy(n).wait()


def per_device(groups, width, *args):
    (source, terminal, jacobian, face_coef, cell_coef, neighbours, send_blocks,
     live_count, volume, shape_field, weights) = args
    steps, nb, comp, cells = source.shape
    nei = face_coef.shape[1]
    count = send_blocks.shape[2]
    edges = 2 * count
    sweeps = steps * ITERS
    f32 = jnp.float32
    bf16 = jnp.bfloat16
    hbm = pl.BlockSpec(memory_space=pltpu.MemorySpace.HBM)
    smem = pl.BlockSpec(memory_space=pltpu.SMEM)
    vmem = pltpu.VMEM
    dma = pltpu.SemaphoreType.DMA
    block = (comp, nb, cells)
    flat = comp * cells
    adjoint, sens = pl.pallas_call(
        functools.partial(kernel, groups, width),
        out_shape=(
            jax.ShapeDtypeStruct((steps, comp, nb, cells), f32),
            jax.ShapeDtypeStruct((1, nb), f32),
        ),
        in_specs=[hbm, hbm, hbm, hbm, hbm, hbm, smem, smem, hbm, hbm, smem],
        out_specs=(hbm, pl.BlockSpec(memory_space=pltpu.VMEM)),
        scratch_shapes=[
            vmem((steps, comp, nb, cells), f32),
            vmem(block, f32),
            vmem((comp, comp, nb, cells), f32),
            vmem((nei, nb, cells), f32),
            vmem((nb, cells), f32),
            vmem((nei, nb), jnp.int32),
            vmem((nb, cells), f32),
            vmem(block, f32),
            vmem(block, f32),
            vmem(block, f32),
            vmem(block, f32),
            vmem(block, f32),
            vmem((nb, cells), f32),
            vmem((nb, cells), f32),
            vmem(block, f32),
            vmem((steps, comp, nb, cells), f32),
            vmem(block, f32),
            vmem((nei * nb, 2 * nb), bf16),
            vmem((nei * nb, nb), bf16),
            vmem((2 * nb, flat), bf16),
            vmem((2 * nb, flat), bf16),
            vmem((nb, flat), bf16),
            vmem((nei * nb, flat), f32),
            vmem((nei * nb, flat), f32),
            vmem((edges, nb), f32),
            vmem((edges, 2 * nb), bf16),
            vmem((nei * edges, nb), bf16),
            vmem((nei, edges, cells), f32),
            vmem((comp, edges, cells), f32),
            vmem((edges, flat), f32),
            vmem((sweeps, 2, comp, count, cells), f32),
            vmem((sweeps, 2, comp, count, cells), f32),
            vmem((8, nb), f32),
            vmem((8, nb), f32),
            vmem((8, nb), f32),
            dma((8,)),
            dma((steps,)),
            dma((sweeps, 2)),
            dma((sweeps, 2)),
            dma,
            dma,
            dma,
            dma,
            dma((groups,)),
            dma,
        ],
        compiler_params=pltpu.CompilerParams(collective_id=0, has_side_effects=True),
    )(
        source.transpose(0, 2, 1, 3),
        terminal.transpose(1, 0, 2),
        jacobian.transpose(0, 2, 3, 1, 4),
        face_coef.transpose(1, 0, 2),
        cell_coef,
        neighbours.T,
        send_blocks,
        live_count,
        volume,
        shape_field.transpose(1, 0, 2),
        weights,
    )
    return adjoint.transpose(0, 2, 1, 3), sens.reshape(nb)


def solution(mesh):
    sizes = dict(mesh.shape)
    return jax.shard_map(
        functools.partial(per_device, sizes["tm"], sizes["space"]),
        mesh=mesh,
        in_specs=(
            P("tm", "space", None, None),
            P("space", None, None),
            P("tm", "space", None, None, None),
            P("space", None, None),
            P("space", None),
            P("space", None),
            P("space", None, None),
            P("space"),
            P("space", None),
            P("space", None, None),
            P("tm"),
        ),
        out_specs=(P("tm", "space", None, None), P("space")),
        check_vma=False,
    )
```

```python
import functools

import jax
import jax.numpy as jnp
from jax import lax
from jax.experimental import pallas as pl
from jax.experimental.pallas import tpu as pltpu
from jax.sharding import PartitionSpec as P

ITERS = 3
INVERSE_STEP = 6.0
TILE = 16
HIGHEST = lax.Precision.HIGHEST


def rows_at(start):
    return pl.ds(start if isinstance(start, int) else pl.multiple_of(start, TILE), TILE)


def split(x):
    high = x.astype(jnp.bfloat16)
    return high, (x - high.astype(jnp.float32)).astype(jnp.bfloat16)


def matmul(a, b, precision=None):
    return jnp.dot(a, b, precision=precision, preferred_element_type=jnp.float32)


def kernel(
    groups,
    width,
    source_hbm,
    terminal_hbm,
    jac_hbm,
    face_hbm,
    cell_hbm,
    nbr_hbm,
    send_blocks,
    live_count,
    volume_hbm,
    shape_hbm,
    weights,
    adjoint_hbm,
    sens_ref,
    source,
    terminal,
    jac,
    face,
    cell,
    nbr,
    volume,
    shape,
    field,
    part,
    rate,
    rate_mass,
    cell_left,
    cell_right,
    rhs,
    levels,
    weighted,
    near_pick,
    far_pick,
    field_terms,
    part_terms,
    halo_terms,
    near,
    far,
    select,
    select_terms,
    edge_pick,
    edge_face,
    edge_rate,
    edge_part,
    halo,
    outbox,
    acc_in,
    acc_out,
    total,
    load_sem,
    store_sem,
    halo_send,
    halo_recv,
    state_send,
    state_recv,
    acc_send,
    acc_recv,
    total_send,
    total_recv,
):
    g = lax.axis_index("tm")
    d = lax.axis_index("space")
    steps, comp, nb, cells = source.shape
    nei = face.shape[0]
    count = outbox.shape[3]
    sweeps = steps * ITERS
    tiles = nb // TILE
    edges = 2 * count
    chunks = [(a, min(a + 2, comp)) for a in range(0, comp, 2)]

    loads = [
        pltpu.make_async_copy(nbr_hbm, nbr, load_sem.at[0]),
        pltpu.make_async_copy(face_hbm, face, load_sem.at[1]),
        pltpu.make_async_copy(cell_hbm, cell, load_sem.at[2]),
        pltpu.make_async_copy(volume_hbm, volume, load_sem.at[3]),
        pltpu.make_async_copy(jac_hbm.at[0], jac, load_sem.at[4]),
        pltpu.make_async_copy(terminal_hbm, terminal, load_sem.at[5]),
        pltpu.make_async_copy(source_hbm, source, load_sem.at[6]),
        pltpu.make_async_copy(shape_hbm, shape, load_sem.at[7]),
    ]
    for load in loads:
        load.start()

    @pl.when((d == 0) | (d == width - 1))
    def _():
        halo[...] = jnp.zeros_like(halo)

    barrier = pltpu.get_barrier_semaphore()
    for other in range(groups):
        @pl.when(g != other)
        def _():
            pl.semaphore_signal(barrier, inc=1, device_id={"tm": other})

    def greet(side):
        pl.semaphore_signal(barrier, inc=1, device_id={"space": side})

        @pl.when(g > 0)
        def _():
            pl.semaphore_signal(barrier, inc=1, device_id={"tm": g - 1, "space": side})

        @pl.when(g < groups - 1)
        def _():
            pl.semaphore_signal(barrier, inc=1, device_id={"tm": g + 1, "space": side})

    @pl.when(d > 0)
    def _():
        greet(d - 1)

    @pl.when(d < width - 1)
    def _():
        greet(d + 1)

    halo_terms[...] = jnp.zeros_like(halo_terms)
    lane = lax.broadcasted_iota(jnp.int32, (1, nb), 1)
    for side in range(2):
        for s in range(count):
            row = side * count + s
            select[pl.ds(row, 1), :] = jnp.where(lane == send_blocks[0, side, s], 1.0, 0.0)
    chosen = select[...]
    chosen_low = chosen.astype(jnp.bfloat16)
    select_terms[:, :nb] = chosen_low
    select_terms[:, nb:] = chosen_low

    loads[0].wait()
    listed = nbr[...].astype(jnp.float32)
    listed = jnp.concatenate([listed, jnp.zeros((nb - nei, nb), jnp.float32)], axis=0).T
    wide = lax.broadcasted_iota(jnp.int32, (nb, nb), 1).astype(jnp.float32)
    for k in range(nei):
        column = jnp.broadcast_to(listed[:, k : k + 1], (nb, nb))
        pick = jnp.where(column == wide, 1.0, 0.0).astype(jnp.bfloat16)
        near_pick[pl.ds(k * nb, nb), :nb] = pick
        near_pick[pl.ds(k * nb, nb), nb:] = pick
        outer = column - nb
        hit = (outer == wide) | (outer + edges == wide)
        inside = (outer >= 0) & (outer < edges)
        pick = jnp.where(hit & inside, 1.0, 0.0).astype(jnp.bfloat16)
        far_pick[pl.ds(k * nb, nb), :] = pick
        edge_pick[pl.ds(k * edges, edges), :] = matmul(chosen_low, pick).astype(jnp.bfloat16)

    for load in loads[1:5]:
        load.wait()
    alive = live_count[0]
    row_id = lax.broadcasted_iota(jnp.int32, (TILE, cells), 0)
    lane_id = lax.broadcasted_iota(jnp.int32, (TILE, cells), 1)

    def live_of(t):
        return jnp.where(row_id + t * TILE < alive, 1.0, 0.0)

    def prepare(t, _):
        r = rows_at(t * TILE)
        live = live_of(t)
        mass = INVERSE_STEP * volume[r, :]
        along = cell[r, :]
        base = mass + 2.0 * along
        for k in range(nei):
            base = base + face[k, r, :]
        cell_left[r, :] = jnp.where(lane_id == 0, 0.0, along)
        cell_right[r, :] = jnp.where(lane_id == cells - 1, 0.0, along)
        for j in range(comp):
            c = live / (base + jac[j, j, r, :])
            rate[j, r, :] = c
            drift = c * mass
            rate_mass[j, r, :] = drift
            for i in range(comp):
                entry = -c * jac[i, j, r, :]
                jac[i, j, r, :] = entry + (live - drift) if i == j else entry
            weighted[j, r, :] = jnp.zeros((TILE, cells), jnp.float32)
        return 0

    lax.fori_loop(0, tiles, prepare, 0)
    for k in range(nei):
        edge_face[k] = matmul(chosen, face[k], HIGHEST)
    for j in range(comp):
        edge_rate[j] = matmul(chosen, rate[j], HIGHEST)

    for load in loads[5:]:
        load.wait()
    sides = jnp.where(d > 0, 1, 0) + jnp.where(d < width - 1, 1, 0)
    slabs = 1 + jnp.where(g > 0, 1, 0) + jnp.where(g < groups - 1, 1, 0)
    pl.semaphore_wait(barrier, groups - 1 + sides * slabs)

    def lanes(j):
        return slice(j * cells, (j + 1) * cells)

    def put_terms(ref, t, j, x):
        high, low = split(x)
        ref[rows_at(t * TILE), lanes(j)] = high
        ref[rows_at(nb + t * TILE), lanes(j)] = low

    def state_copy(to):
        return pltpu.make_async_remote_copy(
            src_ref=field, dst_ref=field, send_sem=state_send, recv_sem=state_recv,
            device_id={"tm": to},
        )

    @pl.when(g == groups - 1)
    def _():
        def begin(t, _):
            r = rows_at(t * TILE)
            for j in range(comp):
                field[j, r, :] = live_of(t) * terminal[j, r, :]
            return 0

        lax.fori_loop(0, tiles, begin, 0)

    @pl.when(g < groups - 1)
    def _():
        state_copy(g).wait_recv()

    def begin_terms(t, _):
        r = rows_at(t * TILE)
        for j in range(comp):
            put_terms(field_terms, t, j, field[j, r, :])
        return 0

    lax.fori_loop(0, tiles, begin_terms, 0)

    def halo_copy(slot, side, c, to):
        own = slot < sweeps
        first, last = chunks[c]
        part_of = pl.ds(first, last - first)
        place = jnp.where(own, slot, 0)
        return pltpu.make_async_remote_copy(
            src_ref=outbox.at[slot, side, part_of],
            dst_ref=halo.at[place, 1 - side, part_of],
            send_sem=halo_send.at[slot, side, c],
            recv_sem=halo_recv.at[place, 1 - side, c],
            device_id={"tm": jnp.where(own, g, g - 1), "space": to},
        )

    def send(slot, c):
        wanted = (slot < sweeps) | (g > 0)

        @pl.when((d > 0) & wanted)
        def _():
            halo_copy(slot, 0, c, d - 1).start()

        @pl.when((d < width - 1) & wanted)
        def _():
            halo_copy(slot, 1, c, d + 1).start()

    def receive(m, c):
        @pl.when(d > 0)
        def _():
            halo_copy(m, 1, c, d - 1).wait_recv()

        @pl.when(d < width - 1)
        def _():
            halo_copy(m, 0, c, d + 1).wait_recv()

    @pl.when(g == groups - 1)
    def _():
        first_out = matmul(select_terms[...], field_terms[...])
        for side in range(2):
            for j in range(comp):
                outbox[0, side, j] = first_out[side * count : (side + 1) * count, lanes(j)]
        for c in range(len(chunks)):
            send(0, c)

    def sweep(m):
        near[...] = matmul(near_pick[...], field_terms[...])

        def local(t, _):
            r = rows_at(t * TILE)
            x = [field[i, r, :] for i in range(comp)]
            left = cell_left[r, :]
            right = cell_right[r, :]
            for j in range(comp):
                value = left * pltpu.roll(x[j], 1, 1) + right * pltpu.roll(x[j], cells - 1, 1)
                for k in range(nei):
                    q = rows_at(k * nb + t * TILE)
                    value = value + face[k, r, :] * near[q, lanes(j)]
                value = rhs[j, r, :] + rate[j, r, :] * value
                for i in range(comp):
                    value = value + jac[i, j, r, :] * x[i]
                part[j, r, :] = value
                put_terms(part_terms, t, j, value)
            return 0

        for t in range(tiles):
            local(t, 0)
        edge_part[...] = matmul(select_terms[...], part_terms[...])
        for c, (first, last) in enumerate(chunks):
            receive(m, c)
            for side in range(2):
                low_rows = slice(edges + side * count, edges + (side + 1) * count)
                for j in range(first, last):
                    high, low = split(halo[m, side, j])
                    halo_terms[side * count : (side + 1) * count, lanes(j)] = high
                    halo_terms[low_rows, lanes(j)] = low
            arrived = matmul(edge_pick[...], halo_terms[:, first * cells : last * cells])
            for side in range(2):
                rows = slice(side * count, (side + 1) * count)
                for j in range(first, last):
                    value = None
                    for k in range(nei):
                        q = slice(k * edges + side * count, k * edges + (side + 1) * count)
                        term = edge_face[k, rows, :] * arrived[q, lanes(j - first)]
                        value = term if value is None else value + term
                    outbox[m + 1, side, j] = edge_part[rows, lanes(j)] + edge_rate[j, rows, :] * value
            send(m + 1, c)

        far[...] = matmul(far_pick[...], halo_terms[...])

        def bulk(t, _):
            r = rows_at(t * TILE)
            for j in range(comp):
                value = None
                for k in range(nei):
                    q = rows_at(k * nb + t * TILE)
                    term = face[k, r, :] * far[q, lanes(j)]
                    value = term if value is None else value + term
                value = part[j, r, :] + rate[j, r, :] * value
                field[j, r, :] = value
                put_terms(field_terms, t, j, value)
            return 0

        for t in range(tiles):
            bulk(t, 0)

    def level_copy(n):
        return pltpu.make_async_copy(levels.at[n], adjoint_hbm.at[n], store_sem.at[n])

    def level(step, _):
        n = steps - 1 - step

        def start(t, _):
            r = rows_at(t * TILE)
            for j in range(comp):
                rhs[j, r, :] = rate[j, r, :] * source[n, j, r, :] + rate_mass[j, r, :] * field[j, r, :]
            return 0

        lax.fori_loop(0, tiles, start, 0)

        def inner(it, _):
            sweep(step * ITERS + it)
            return 0

        lax.fori_loop(0, ITERS, inner, 0)

        @pl.when((step == steps - 1) & (g > 0))
        def _():
            state_copy(g - 1).start()

        weight = weights[n]

        def finish(t, _):
            r = rows_at(t * TILE)
            for j in range(comp):
                x = field[j, r, :]
                levels[n, j, r, :] = x
                weighted[j, r, :] = weighted[j, r, :] + weight * x
            return 0

        lax.fori_loop(0, tiles, finish, 0)
        level_copy(n).start()
        return 0

    lax.fori_loop(0, steps, level, 0)

    summed = jnp.zeros((nb, cells), jnp.float32)
    for j in range(comp):
        summed = summed + weighted[j] * shape[j]

    mine = lax.dot_general(
        jnp.ones((8, cells), jnp.float32),
        summed,
        (((1,), (1,)), ((), ())),
        precision=lax.Precision.HIGHEST,
        preferred_element_type=jnp.float32,
    )

    def acc_copy(to):
        return pltpu.make_async_remote_copy(
            src_ref=acc_out, dst_ref=acc_in, send_sem=acc_send, recv_sem=acc_recv,
            device_id={"tm": to},
        )

    def total_copy(to):
        return pltpu.make_async_remote_copy(
            src_ref=acc_out, dst_ref=total, send_sem=total_send.at[to], recv_sem=total_recv,
            device_id={"tm": to},
        )

    @pl.when(g == groups - 1)
    def _():
        acc_out[...] = mine

    @pl.when(g < groups - 1)
    def _():
        acc_copy(g).wait_recv()
        acc_out[...] = mine + acc_in[...]

    @pl.when(g > 0)
    def _():
        acc_copy(g - 1).start()
        total_copy(g).wait_recv()
        sens_ref[...] = total[0:1, :]

    @pl.when(g == 0)
    def _():
        for other in range(1, groups):
            total_copy(other).start()
        sens_ref[...] = acc_out[0:1, :]
        for other in range(1, groups):
            total_copy(other).wait_send()

    @pl.when(g > 0)
    def _():
        acc_copy(g - 1).wait_send()
        state_copy(g - 1).wait_send()

    def drain(slot, _):
        wanted = ((slot > 0) | (g == groups - 1)) & ((slot < sweeps) | (g > 0))
        for c in range(len(chunks)):
            @pl.when((d > 0) & wanted)
            def _():
                halo_copy(slot, 0, c, d - 1).wait_send()

            @pl.when((d < width - 1) & wanted)
            def _():
                halo_copy(slot, 1, c, d + 1).wait_send()

        return 0

    lax.fori_loop(0, sweeps + 1, drain, 0)
    for n in range(steps):
        level_copy(n).wait()


def per_device(groups, width, *args):
    (source, terminal, jacobian, face_coef, cell_coef, neighbours, send_blocks,
     live_count, volume, shape_field, weights) = args
    steps, nb, comp, cells = source.shape
    nei = face_coef.shape[1]
    count = send_blocks.shape[2]
    edges = 2 * count
    sweeps = steps * ITERS
    f32 = jnp.float32
    bf16 = jnp.bfloat16
    hbm = pl.BlockSpec(memory_space=pltpu.MemorySpace.HBM)
    smem = pl.BlockSpec(memory_space=pltpu.SMEM)
    vmem = pltpu.VMEM
    dma = pltpu.SemaphoreType.DMA
    block = (comp, nb, cells)
    flat = comp * cells
    chunks = -(-comp // 2)
    adjoint, sens = pl.pallas_call(
        functools.partial(kernel, groups, width),
        out_shape=(
            jax.ShapeDtypeStruct((steps, comp, nb, cells), f32),
            jax.ShapeDtypeStruct((1, nb), f32),
        ),
        in_specs=[hbm, hbm, hbm, hbm, hbm, hbm, smem, smem, hbm, hbm, smem],
        out_specs=(hbm, pl.BlockSpec(memory_space=pltpu.VMEM)),
        scratch_shapes=[
            vmem((steps, comp, nb, cells), f32),
            vmem(block, f32),
            vmem((comp, comp, nb, cells), f32),
            vmem((nei, nb, cells), f32),
            vmem((nb, cells), f32),
            vmem((nei, nb), jnp.int32),
            vmem((nb, cells), f32),
            vmem(block, f32),
            vmem(block, f32),
            vmem(block, f32),
            vmem(block, f32),
            vmem(block, f32),
            vmem((nb, cells), f32),
            vmem((nb, cells), f32),
            vmem(block, f32),
            vmem((steps, comp, nb, cells), f32),
            vmem(block, f32),
            vmem((nei * nb, 2 * nb), bf16),
            vmem((nei * nb, nb), bf16),
            vmem((2 * nb, flat), bf16),
            vmem((2 * nb, flat), bf16),
            vmem((nb, flat), bf16),
            vmem((nei * nb, flat), f32),
            vmem((nei * nb, flat), f32),
            vmem((edges, nb), f32),
            vmem((edges, 2 * nb), bf16),
            vmem((nei * edges, nb), bf16),
            vmem((nei, edges, cells), f32),
            vmem((comp, edges, cells), f32),
            vmem((edges, flat), f32),
            vmem((sweeps, 2, comp, count, cells), f32),
            vmem((sweeps + 1, 2, comp, count, cells), f32),
            vmem((8, nb), f32),
            vmem((8, nb), f32),
            vmem((8, nb), f32),
            dma((8,)),
            dma((steps,)),
            dma((sweeps + 1, 2, chunks)),
            dma((sweeps, 2, chunks)),
            dma,
            dma,
            dma,
            dma,
            dma((groups,)),
            dma,
        ],
        compiler_params=pltpu.CompilerParams(collective_id=0, has_side_effects=True),
    )(
        source.transpose(0, 2, 1, 3),
        terminal.transpose(1, 0, 2),
        jacobian.transpose(0, 2, 3, 1, 4),
        face_coef.transpose(1, 0, 2),
        cell_coef,
        neighbours.T,
        send_blocks,
        live_count,
        volume,
        shape_field.transpose(1, 0, 2),
        weights,
    )
    return adjoint.transpose(0, 2, 1, 3), sens.reshape(nb)


def solution(mesh):
    sizes = dict(mesh.shape)
    return jax.shard_map(
        functools.partial(per_device, sizes["tm"], sizes["space"]),
        mesh=mesh,
        in_specs=(
            P("tm", "space", None, None),
            P("space", None, None),
            P("tm", "space", None, None, None),
            P("space", None, None),
            P("space", None),
            P("space", None),
            P("space", None, None),
            P("space"),
            P("space", None),
            P("space", None, None),
            P("tm"),
        ),
        out_specs=(P("tm", "space", None, None), P("space")),
        check_vma=False,
    )
```

```python
import functools

import jax
import jax.numpy as jnp
from jax import lax
from jax.experimental import pallas as pl
from jax.experimental.pallas import tpu as pltpu
from jax.sharding import PartitionSpec as P

ITERS = 3
INVERSE_STEP = 6.0
TILE = 16
HIGHEST = lax.Precision.HIGHEST


def rows_at(start):
    return pl.ds(start if isinstance(start, int) else pl.multiple_of(start, TILE), TILE)


def split(x):
    high = x.astype(jnp.bfloat16)
    return high, (x - high.astype(jnp.float32)).astype(jnp.bfloat16)


def matmul(a, b, precision=None):
    return jnp.dot(a, b, precision=precision, preferred_element_type=jnp.float32)


def kernel(
    groups,
    width,
    source_hbm,
    terminal_hbm,
    jac_hbm,
    face_hbm,
    cell_hbm,
    nbr_hbm,
    send_blocks,
    live_count,
    volume_hbm,
    shape_hbm,
    weights,
    adjoint_hbm,
    sens_ref,
    source,
    terminal,
    jac,
    face,
    cell,
    nbr,
    volume,
    shape,
    field,
    part,
    rate,
    rate_mass,
    cell_left,
    cell_right,
    rhs,
    levels,
    weighted,
    near_pick,
    far_pick,
    field_terms,
    part_terms,
    halo_terms,
    near,
    far,
    select,
    select_terms,
    edge_pick,
    edge_face,
    edge_rate,
    edge_part,
    halo,
    outbox,
    acc_in,
    acc_out,
    total,
    load_sem,
    store_sem,
    halo_send,
    halo_recv,
    state_send,
    state_recv,
    acc_send,
    acc_recv,
    total_send,
    total_recv,
):
    g = lax.axis_index("tm")
    d = lax.axis_index("space")
    steps, comp, nb, cells = source.shape
    nei = face.shape[0]
    count = outbox.shape[3]
    sweeps = steps * ITERS
    tiles = nb // TILE
    edges = 2 * count
    chunks = [(a, min(a + 2, comp)) for a in range(0, comp, 2)]

    loads = [
        pltpu.make_async_copy(nbr_hbm, nbr, load_sem.at[0]),
        pltpu.make_async_copy(face_hbm, face, load_sem.at[1]),
        pltpu.make_async_copy(cell_hbm, cell, load_sem.at[2]),
        pltpu.make_async_copy(volume_hbm, volume, load_sem.at[3]),
        pltpu.make_async_copy(jac_hbm.at[0], jac, load_sem.at[4]),
        pltpu.make_async_copy(terminal_hbm, terminal, load_sem.at[5]),
        pltpu.make_async_copy(source_hbm, source, load_sem.at[6]),
        pltpu.make_async_copy(shape_hbm, shape, load_sem.at[7]),
    ]
    for load in loads:
        load.start()

    @pl.when((d == 0) | (d == width - 1))
    def _():
        halo[...] = jnp.zeros_like(halo)

    barrier = pltpu.get_barrier_semaphore()
    for other in range(groups):
        @pl.when(g != other)
        def _():
            pl.semaphore_signal(barrier, inc=1, device_id={"tm": other})

    def greet(side):
        pl.semaphore_signal(barrier, inc=1, device_id={"space": side})

        @pl.when(g > 0)
        def _():
            pl.semaphore_signal(barrier, inc=1, device_id={"tm": g - 1, "space": side})

        @pl.when(g < groups - 1)
        def _():
            pl.semaphore_signal(barrier, inc=1, device_id={"tm": g + 1, "space": side})

    @pl.when(d > 0)
    def _():
        greet(d - 1)

    @pl.when(d < width - 1)
    def _():
        greet(d + 1)

    halo_terms[...] = jnp.zeros_like(halo_terms)
    lane = lax.broadcasted_iota(jnp.int32, (1, nb), 1)
    for side in range(2):
        for s in range(count):
            row = side * count + s
            select[pl.ds(row, 1), :] = jnp.where(lane == send_blocks[0, side, s], 1.0, 0.0)
    chosen = select[...]
    chosen_low = chosen.astype(jnp.bfloat16)
    select_terms[:, :nb] = chosen_low
    select_terms[:, nb:] = chosen_low

    loads[0].wait()
    listed = nbr[...].astype(jnp.float32)
    listed = jnp.concatenate([listed, jnp.zeros((nb - nei, nb), jnp.float32)], axis=0).T
    wide = lax.broadcasted_iota(jnp.int32, (nb, nb), 1).astype(jnp.float32)
    for k in range(nei):
        column = jnp.broadcast_to(listed[:, k : k + 1], (nb, nb))
        pick = jnp.where(column == wide, 1.0, 0.0).astype(jnp.bfloat16)
        near_pick[pl.ds(k * nb, nb), :nb] = pick
        near_pick[pl.ds(k * nb, nb), nb:] = pick
        outer = column - nb
        hit = (outer == wide) | (outer + edges == wide)
        inside = (outer >= 0) & (outer < edges)
        pick = jnp.where(hit & inside, 1.0, 0.0).astype(jnp.bfloat16)
        far_pick[pl.ds(k * nb, nb), :] = pick
        edge_pick[pl.ds(k * edges, edges), :] = matmul(chosen_low, pick).astype(jnp.bfloat16)

    for load in loads[1:5]:
        load.wait()
    alive = live_count[0]
    row_id = lax.broadcasted_iota(jnp.int32, (TILE, cells), 0)
    lane_id = lax.broadcasted_iota(jnp.int32, (TILE, cells), 1)

    def live_of(t):
        return jnp.where(row_id + t * TILE < alive, 1.0, 0.0)

    def prepare(t, _):
        r = rows_at(t * TILE)
        live = live_of(t)
        mass = INVERSE_STEP * volume[r, :]
        along = cell[r, :]
        base = mass + 2.0 * along
        for k in range(nei):
            base = base + face[k, r, :]
        cell_left[r, :] = jnp.where(lane_id == 0, 0.0, along)
        cell_right[r, :] = jnp.where(lane_id == cells - 1, 0.0, along)
        for j in range(comp):
            c = live / (base + jac[j, j, r, :])
            rate[j, r, :] = c
            drift = c * mass
            rate_mass[j, r, :] = drift
            for i in range(comp):
                entry = -c * jac[i, j, r, :]
                jac[i, j, r, :] = entry + (live - drift) if i == j else entry
            weighted[j, r, :] = jnp.zeros((TILE, cells), jnp.float32)
        return 0

    for t in range(tiles):
        prepare(t, 0)
    for k in range(nei):
        edge_face[k] = matmul(chosen, face[k], HIGHEST)
    for j in range(comp):
        edge_rate[j] = matmul(chosen, rate[j], HIGHEST)

    for load in loads[5:]:
        load.wait()
    sides = jnp.where(d > 0, 1, 0) + jnp.where(d < width - 1, 1, 0)
    slabs = 1 + jnp.where(g > 0, 1, 0) + jnp.where(g < groups - 1, 1, 0)
    pl.semaphore_wait(barrier, groups - 1 + sides * slabs)

    def lanes(j):
        return slice(j * cells, (j + 1) * cells)

    def put_terms(ref, t, j, x):
        high, low = split(x)
        ref[rows_at(t * TILE), lanes(j)] = high
        ref[rows_at(nb + t * TILE), lanes(j)] = low

    def state_copy(to):
        return pltpu.make_async_remote_copy(
            src_ref=field, dst_ref=field, send_sem=state_send, recv_sem=state_recv,
            device_id={"tm": to},
        )

    @pl.when(g == groups - 1)
    def _():
        def begin(t, _):
            r = rows_at(t * TILE)
            for j in range(comp):
                field[j, r, :] = live_of(t) * terminal[j, r, :]
            return 0

        for t in range(tiles):
            begin(t, 0)

    @pl.when(g < groups - 1)
    def _():
        state_copy(g).wait_recv()

    def begin_terms(t, _):
        r = rows_at(t * TILE)
        for j in range(comp):
            put_terms(field_terms, t, j, field[j, r, :])
        return 0

    for t in range(tiles):
        begin_terms(t, 0)

    def halo_copy(slot, side, c, to):
        own = slot < sweeps
        first, last = chunks[c]
        part_of = pl.ds(first, last - first)
        place = jnp.where(own, slot, 0)
        return pltpu.make_async_remote_copy(
            src_ref=outbox.at[slot, side, part_of],
            dst_ref=halo.at[place, 1 - side, part_of],
            send_sem=halo_send.at[slot, side, c],
            recv_sem=halo_recv.at[place, 1 - side, c],
            device_id={"tm": jnp.where(own, g, g - 1), "space": to},
        )

    def send(slot, c):
        wanted = (slot < sweeps) | (g > 0)

        @pl.when((d > 0) & wanted)
        def _():
            halo_copy(slot, 0, c, d - 1).start()

        @pl.when((d < width - 1) & wanted)
        def _():
            halo_copy(slot, 1, c, d + 1).start()

    def receive(m, c):
        @pl.when(d > 0)
        def _():
            halo_copy(m, 1, c, d - 1).wait_recv()

        @pl.when(d < width - 1)
        def _():
            halo_copy(m, 0, c, d + 1).wait_recv()

    @pl.when(g == groups - 1)
    def _():
        first_out = matmul(select_terms[...], field_terms[...])
        for side in range(2):
            for j in range(comp):
                outbox[0, side, j] = first_out[side * count : (side + 1) * count, lanes(j)]
        for c in range(len(chunks)):
            send(0, c)

    def sweep(m):
        near[...] = matmul(near_pick[...], field_terms[...])

        def local(t, _):
            r = rows_at(t * TILE)
            x = [field[i, r, :] for i in range(comp)]
            left = cell_left[r, :]
            right = cell_right[r, :]
            for j in range(comp):
                value = left * pltpu.roll(x[j], 1, 1) + right * pltpu.roll(x[j], cells - 1, 1)
                for k in range(nei):
                    q = rows_at(k * nb + t * TILE)
                    value = value + face[k, r, :] * near[q, lanes(j)]
                value = rhs[j, r, :] + rate[j, r, :] * value
                for i in range(comp):
                    value = value + jac[i, j, r, :] * x[i]
                part[j, r, :] = value
                put_terms(part_terms, t, j, value)
            return 0

        for t in range(tiles):
            local(t, 0)
        edge_part[...] = matmul(select_terms[...], part_terms[...])
        for c, (first, last) in enumerate(chunks):
            receive(m, c)
            for side in range(2):
                low_rows = slice(edges + side * count, edges + (side + 1) * count)
                for j in range(first, last):
                    high, low = split(halo[m, side, j])
                    halo_terms[side * count : (side + 1) * count, lanes(j)] = high
                    halo_terms[low_rows, lanes(j)] = low
            arrived = matmul(edge_pick[...], halo_terms[:, first * cells : last * cells])
            for side in range(2):
                rows = slice(side * count, (side + 1) * count)
                for j in range(first, last):
                    value = None
                    for k in range(nei):
                        q = slice(k * edges + side * count, k * edges + (side + 1) * count)
                        term = edge_face[k, rows, :] * arrived[q, lanes(j - first)]
                        value = term if value is None else value + term
                    outbox[m + 1, side, j] = edge_part[rows, lanes(j)] + edge_rate[j, rows, :] * value
            send(m + 1, c)

        far[...] = matmul(far_pick[...], halo_terms[...])

        def bulk(t, _):
            r = rows_at(t * TILE)
            for j in range(comp):
                value = None
                for k in range(nei):
                    q = rows_at(k * nb + t * TILE)
                    term = face[k, r, :] * far[q, lanes(j)]
                    value = term if value is None else value + term
                value = part[j, r, :] + rate[j, r, :] * value
                field[j, r, :] = value
                put_terms(field_terms, t, j, value)
            return 0

        for t in range(tiles):
            bulk(t, 0)

    def level_copy(n):
        return pltpu.make_async_copy(levels.at[n], adjoint_hbm.at[n], store_sem.at[n])

    def level(step, _):
        n = steps - 1 - step

        def start(t, _):
            r = rows_at(t * TILE)
            for j in range(comp):
                rhs[j, r, :] = rate[j, r, :] * source[n, j, r, :] + rate_mass[j, r, :] * field[j, r, :]
            return 0

        for t in range(tiles):
            start(t, 0)

        def inner(it, _):
            sweep(step * ITERS + it)
            return 0

        lax.fori_loop(0, ITERS, inner, 0)

        @pl.when((step == steps - 1) & (g > 0))
        def _():
            state_copy(g - 1).start()

        weight = weights[n]

        def finish(t, _):
            r = rows_at(t * TILE)
            for j in range(comp):
                x = field[j, r, :]
                levels[n, j, r, :] = x
                weighted[j, r, :] = weighted[j, r, :] + weight * x
            return 0

        for t in range(tiles):
            finish(t, 0)
        level_copy(n).start()
        return 0

    lax.fori_loop(0, steps, level, 0)

    summed = jnp.zeros((nb, cells), jnp.float32)
    for j in range(comp):
        summed = summed + weighted[j] * shape[j]

    mine = lax.dot_general(
        jnp.ones((8, cells), jnp.float32),
        summed,
        (((1,), (1,)), ((), ())),
        precision=lax.Precision.HIGHEST,
        preferred_element_type=jnp.float32,
    )

    def acc_copy(to):
        return pltpu.make_async_remote_copy(
            src_ref=acc_out, dst_ref=acc_in, send_sem=acc_send, recv_sem=acc_recv,
            device_id={"tm": to},
        )

    def total_copy(to):
        return pltpu.make_async_remote_copy(
            src_ref=acc_out, dst_ref=total, send_sem=total_send.at[to], recv_sem=total_recv,
            device_id={"tm": to},
        )

    @pl.when(g == groups - 1)
    def _():
        acc_out[...] = mine

    @pl.when(g < groups - 1)
    def _():
        acc_copy(g).wait_recv()
        acc_out[...] = mine + acc_in[...]

    @pl.when(g > 0)
    def _():
        acc_copy(g - 1).start()
        total_copy(g).wait_recv()
        sens_ref[...] = total[0:1, :]

    @pl.when(g == 0)
    def _():
        for other in range(1, groups):
            total_copy(other).start()
        sens_ref[...] = acc_out[0:1, :]
        for other in range(1, groups):
            total_copy(other).wait_send()

    @pl.when(g > 0)
    def _():
        acc_copy(g - 1).wait_send()
        state_copy(g - 1).wait_send()

    def drain(slot, _):
        wanted = ((slot > 0) | (g == groups - 1)) & ((slot < sweeps) | (g > 0))
        for c in range(len(chunks)):
            @pl.when((d > 0) & wanted)
            def _():
                halo_copy(slot, 0, c, d - 1).wait_send()

            @pl.when((d < width - 1) & wanted)
            def _():
                halo_copy(slot, 1, c, d + 1).wait_send()

        return 0

    lax.fori_loop(0, sweeps + 1, drain, 0)
    for n in range(steps):
        level_copy(n).wait()


def per_device(groups, width, *args):
    (source, terminal, jacobian, face_coef, cell_coef, neighbours, send_blocks,
     live_count, volume, shape_field, weights) = args
    steps, nb, comp, cells = source.shape
    nei = face_coef.shape[1]
    count = send_blocks.shape[2]
    edges = 2 * count
    sweeps = steps * ITERS
    f32 = jnp.float32
    bf16 = jnp.bfloat16
    hbm = pl.BlockSpec(memory_space=pltpu.MemorySpace.HBM)
    smem = pl.BlockSpec(memory_space=pltpu.SMEM)
    vmem = pltpu.VMEM
    dma = pltpu.SemaphoreType.DMA
    block = (comp, nb, cells)
    flat = comp * cells
    chunks = -(-comp // 2)
    adjoint, sens = pl.pallas_call(
        functools.partial(kernel, groups, width),
        out_shape=(
            jax.ShapeDtypeStruct((steps, comp, nb, cells), f32),
            jax.ShapeDtypeStruct((1, nb), f32),
        ),
        in_specs=[hbm, hbm, hbm, hbm, hbm, hbm, smem, smem, hbm, hbm, smem],
        out_specs=(hbm, pl.BlockSpec(memory_space=pltpu.VMEM)),
        scratch_shapes=[
            vmem((steps, comp, nb, cells), f32),
            vmem(block, f32),
            vmem((comp, comp, nb, cells), f32),
            vmem((nei, nb, cells), f32),
            vmem((nb, cells), f32),
            vmem((nei, nb), jnp.int32),
            vmem((nb, cells), f32),
            vmem(block, f32),
            vmem(block, f32),
            vmem(block, f32),
            vmem(block, f32),
            vmem(block, f32),
            vmem((nb, cells), f32),
            vmem((nb, cells), f32),
            vmem(block, f32),
            vmem((steps, comp, nb, cells), f32),
            vmem(block, f32),
            vmem((nei * nb, 2 * nb), bf16),
            vmem((nei * nb, nb), bf16),
            vmem((2 * nb, flat), bf16),
            vmem((2 * nb, flat), bf16),
            vmem((nb, flat), bf16),
            vmem((nei * nb, flat), f32),
            vmem((nei * nb, flat), f32),
            vmem((edges, nb), f32),
            vmem((edges, 2 * nb), bf16),
            vmem((nei * edges, nb), bf16),
            vmem((nei, edges, cells), f32),
            vmem((comp, edges, cells), f32),
            vmem((edges, flat), f32),
            vmem((sweeps, 2, comp, count, cells), f32),
            vmem((sweeps + 1, 2, comp, count, cells), f32),
            vmem((8, nb), f32),
            vmem((8, nb), f32),
            vmem((8, nb), f32),
            dma((8,)),
            dma((steps,)),
            dma((sweeps + 1, 2, chunks)),
            dma((sweeps, 2, chunks)),
            dma,
            dma,
            dma,
            dma,
            dma((groups,)),
            dma,
        ],
        compiler_params=pltpu.CompilerParams(collective_id=0, has_side_effects=True),
    )(
        source.transpose(0, 2, 1, 3),
        terminal.transpose(1, 0, 2),
        jacobian.transpose(0, 2, 3, 1, 4),
        face_coef.transpose(1, 0, 2),
        cell_coef,
        neighbours.T,
        send_blocks,
        live_count,
        volume,
        shape_field.transpose(1, 0, 2),
        weights,
    )
    return adjoint.transpose(0, 2, 1, 3), sens.reshape(nb)


def solution(mesh):
    sizes = dict(mesh.shape)
    return jax.shard_map(
        functools.partial(per_device, sizes["tm"], sizes["space"]),
        mesh=mesh,
        in_specs=(
            P("tm", "space", None, None),
            P("space", None, None),
            P("tm", "space", None, None, None),
            P("space", None, None),
            P("space", None),
            P("space", None),
            P("space", None, None),
            P("space"),
            P("space", None),
            P("space", None, None),
            P("tm"),
        ),
        out_specs=(P("tm", "space", None, None), P("space")),
        check_vma=False,
    )
```
